256 devices in a mesh: pop: 32 (over x, z), grp: 8 (over y, core).
Axes of the slice: x: 4, y: 4, z: 8, core: 2. Of those that a mesh axis runs over, the one named last changes fastest.
Arguments:
- actions: bfloat16 [131072, 1024], P(('pop', 'grp')), may hold values from -24 to 24
- elite_mask: int32 [131072], P(('pop', 'grp')), may hold values from 0 to 1, as said below
- init_state: float32 [256], replicated, may hold values from -6 to 6
- w_state: bfloat16 [256, 256], replicated, may hold values from -0.375 to 0.375
- w_action: bfloat16 [32, 256], replicated, may hold values from -1 to 1
- bias: float32 [256], replicated, may hold values from -3 to 3
- w_out: bfloat16 [256, 256], replicated, may hold values from -0.375 to 0.375
- reward_vec: float32 [256], replicated, may hold values from -0.375 to 0.375
Outputs:
- new_mean: float32 [1024], replicated
- covariance: float32 [1024, 1024], P('pop')
- returns: float32 [131072], P(('pop', 'grp'))
The draws below stay inside these ranges and needn't reach their ends.
Inputs may be any that keep to these rules, and one draw needn't show every extreme that they name: `elite_mask`: each aligned block of 512 candidates (the candidates of one device) holds at least one elite.
All inputs are finite; a program needn't handle non-finite values.
Results may differ from the reference program's by a relative error of at most 0.0063.
Values sent between devices are 32-bit elements; how exact they have to be, the bound alone decides.
A program may use at most 64 MiB of HBM per device.

```python
import jax
import jax.numpy as jnp
from jax import lax

ACT = 32
STEPS = 32
STATE = 256
HIDDEN_SIZE = 256
CAND_DEV = 512
DIM = 1024
POP = 131072


def draw_elite_mask(key, part):
    base = jax.random.randint(jax.random.fold_in(key, 11), (POP,), 0, 8)
    chosen = jax.random.randint(jax.random.fold_in(key, 12), (POP // CAND_DEV, 1), 0, CAND_DEV)
    position = jnp.arange(CAND_DEV, dtype=jnp.int32)[None, :]
    forced = (position == chosen).reshape(POP)
    return jnp.where(forced | (base == 0), 1, 0).astype(jnp.int32)


def raised(entries, rng, source, target, parts, factor):
    def block_of(axis_at):
        return (jnp.arange(entries.shape[axis_at]) // (entries.shape[axis_at] // parts)).reshape((-1,) + (1,) * (entries.ndim - 1 - axis_at))

    one_side = jax.random.permutation(rng, parts)[block_of(target)]
    second = (block_of(target) + parts // 2) % parts
    return jnp.where((block_of(source) == one_side) | (block_of(source) == second), factor * entries, entries)


def block_scale(key, extent, split, low, top_value):
    gain, own = 1.0, jax.random.fold_in(key, 6)
    for dim, parts in split:
        heights = jnp.exp(jax.random.uniform(jax.random.fold_in(own, dim), (parts,), jnp.float32, low / len(split), top_value / len(split)))
        gain = gain * jnp.repeat(heights, extent[dim] // parts).reshape([-1 if axis == dim else 1 for axis in range(len(extent))])
    return gain


def scatter_about(rng, dims, scale, limit, split=(), kind=jnp.bfloat16):
    drawn = jax.random.normal(rng, dims, jnp.float32) * scale
    if len(split) > 0:
        drawn = block_scale(rng, dims, split, -0.22, 0.18) * drawn
    return jnp.clip(drawn, min=-limit, max=limit).astype(kind)


def heavy_noise(stream_key, extent, width, most, pieces, heavy, held_as=jnp.bfloat16):
    entries = width * jax.random.normal(stream_key, extent, jnp.float32)
    if pieces:
        entries = entries * block_scale(stream_key, extent, pieces, -0.22, 0.18)
    return jnp.clip(raised(entries, jax.random.fold_in(stream_key, 3), *heavy), -most, most).astype(held_as)


def setup_inputs(seed: int = 0) -> dict:
    keys = jax.random.split(jax.random.key(seed), 9)
    return {
        "actions": heavy_noise(keys[0], (POP, DIM), 1.0, 24.0, ((0, 256),), (0, 1, 256, 6.0)),
        "elite_mask": draw_elite_mask(jax.random.fold_in(keys[8], 71), 0),
        "init_state": scatter_about(keys[2], (STATE,), 1.0, 6.0, (), jnp.float32),
        "w_state": scatter_about(keys[3], (STATE, HIDDEN_SIZE), STATE ** -0.5, 0.375),
        "w_action": scatter_about(keys[4], (ACT, HIDDEN_SIZE), ACT ** -0.5, 1.0),
        "bias": scatter_about(keys[5], (HIDDEN_SIZE,), 0.5, 3.0, (), jnp.float32),
        "w_out": scatter_about(keys[6], (HIDDEN_SIZE, STATE), HIDDEN_SIZE ** -0.5, 0.375),
        "reward_vec": scatter_about(keys[7], (STATE,), STATE ** -0.5, 0.375, (), jnp.float32),
    }


def reference(actions, elite_mask, init_state, w_state, w_action, bias, w_out, reward_vec):
    weight = elite_mask.astype(jnp.float32)
    weight_b = weight.astype(jnp.bfloat16)
    count = jnp.sum(weight)
    sums = jnp.dot(weight_b[None, :], actions, preferred_element_type=jnp.float32)[0]
    new_mean = sums / count
    masked = actions * weight_b[:, None]
    second = lax.dot_general(masked, actions, (((0,), (0,)), ((), ())), preferred_element_type=jnp.float32)
    covariance = second / count - new_mean[:, None] * new_mean[None, :]
    total_rows = actions.shape[0]
    per_step = jnp.transpose(actions.reshape(total_rows, STEPS, ACT), (1, 0, 2))
    start = jnp.broadcast_to(init_state[None, :], (total_rows, STATE)).astype(jnp.float32)

    def advance(carry, action_now):
        state, total = carry
        state_b = state.astype(jnp.bfloat16)
        pre = jnp.dot(state_b, w_state, preferred_element_type=jnp.float32)
        pre = pre + jnp.dot(action_now, w_action, preferred_element_type=jnp.float32) + bias
        hidden = jnp.tanh(pre).astype(jnp.bfloat16)
        state = 0.9 * state + jnp.dot(hidden, w_out, preferred_element_type=jnp.float32)
        total = total + jnp.sum(state * reward_vec[None, :], axis=1)
        return (state, total), None

    (final, total), unused = lax.scan(advance, (start, jnp.zeros((total_rows,), jnp.float32)), per_step)
    returns = total / STEPS
    return new_mean, covariance, returns
```

```python
import functools

import jax
import jax.numpy as jnp
from jax import lax
from jax.experimental import pallas as pl
from jax.experimental.pallas import tpu as pltpu
from jax.sharding import Mesh
from jax.sharding import PartitionSpec as P

ACT = 32
STEPS = 32
STATE = 256
DIM = 1024
MESH = pl.DeviceIdType.MESH
AXES = ("x", "z", "y", "c")
NX, NZ, NY = 4, 8, 4
HALF = DIM // 2
PACK = 128 // ACT
FILL = (1, 2, 2, 1, 1, 1, 0)


def kernel(
    act_ref, mask_ref, init_ref, ws_ref, wa_ref, bias_ref, wo_ref, rv_ref,
    mean_ref, cov_ref, ret_ref,
    part, own, b1p, b1m, bdp, bdm, b2p, b2m, mid, c1p, c1m, cdp, cdm, c2p, c2m, low, zin, gath,
    s_c, s_x, s_y, s_z, wa_pad, state, acc,
    pair_send, pair_recv, r1_send, r1_recv, r2_send, r2_recv, z_send, z_recv, g_send, g_recv,
    sc_send, sc_recv, sx_send, sx_recv, sy_send, sy_recv, sz_send, sz_recv,
):
    x, z, y, c = (lax.axis_index(a) for a in AXES)
    sib = 1 - c
    f32, bf16 = jnp.float32, jnp.bfloat16

    def copy(src, dst, ssem, rsem, **where):
        return pltpu.make_async_remote_copy(
            src_ref=src, dst_ref=dst, send_sem=ssem, recv_sem=rsem,
            device_id=where, device_id_type=MESH,
        )

    barrier = pltpu.get_barrier_semaphore()

    def greet(**where):
        pl.semaphore_signal(barrier, inc=1, device_id=where, device_id_type=MESH)

    greet(c=sib)
    for d in range(1, NX):
        greet(x=lax.rem(x + d, NX))
    for d in range(1, NY):
        greet(y=lax.rem(y + d, NY))
        greet(y=lax.rem(y + d, NY), c=sib)
    for d in range(1, NZ):
        greet(z=lax.rem(z + d, NZ))

    wa_pad[...] = jnp.zeros_like(wa_pad)
    for j in range(PACK):
        wa_pad[j, j * ACT:(j + 1) * ACT, :] = wa_ref[...]
    state[...] = jnp.broadcast_to(init_ref[...], state.shape)
    acc[...] = jnp.zeros_like(acc)

    def rollout(first, count):
        @pl.loop(first, first + count)
        def _(g):
            block = act_ref[:, pl.ds(pl.multiple_of(g * 128, 128), 128)]
            for j in range(PACK):
                st = state[...]
                pre = jnp.dot(st.astype(bf16), ws_ref[...], preferred_element_type=f32)
                pre = pre + jnp.dot(block, wa_pad[j], preferred_element_type=f32) + bias_ref[...]
                hidden = jnp.tanh(pre).astype(bf16)
                st = 0.9 * st + jnp.dot(hidden, wo_ref[...], preferred_element_type=f32)
                state[...] = st
                acc[...] += st

    done = 0

    def fill(k):
        nonlocal done
        n = min(FILL[k], STEPS // PACK - done)
        if n > 0:
            rollout(done, n)
        done += n

    w_i = mask_ref[...]
    w_row = w_i.astype(f32)
    w_b = w_row.astype(bf16)
    sums = jnp.dot(jnp.broadcast_to(w_b, (16, w_b.shape[1])), act_ref[...], preferred_element_type=f32)
    s_c[c, 0:1, :] = sums[0:1]
    s_c[c, 1:2, :] = jnp.broadcast_to(jnp.sum(w_row, axis=1, keepdims=True), (1, DIM))

    pair = []
    side = pl.ds(pl.multiple_of(sib * HALF, HALF), HALF)
    mine = pl.ds(pl.multiple_of(c * HALF, HALF), HALF)
    for xs in range(NX):
        at = act_ref[:, xs * 256:(xs + 1) * 256].T * w_b
        prod = jnp.dot(at, act_ref[...], preferred_element_type=f32)
        part[xs] = prod.reshape(NZ, NY, 8, DIM)
        if xs == 0:
            pl.semaphore_wait(barrier, (NX - 1) + 2 * (NY - 1) + (NZ - 1) + 1)
            sc = copy(s_c.at[c], s_c.at[c], sc_send, sc_recv, c=sib)
            sc.start()
        for ys in range(NY):
            a = xs * (1 - sib) + ys * sib
            b = ys * (1 - sib) + xs * sib
            k = a * 4 + b
            cp = copy(part.at[xs, :, ys, :, side], own.at[a, b], pair_send.at[k], pair_recv.at[k], c=sib)
            cp.start()
            pair.append(cp)

    fill(0)

    def take(a, b):
        k = a * 4 + b
        copy(part.at[0, :, 0, :, side], own.at[a, b], pair_send.at[k], pair_recv.at[k], c=sib).wait_recv()
        xs = a * (1 - c) + b * c
        ys = b * (1 - c) + a * c
        own[a, b] = own[a, b] + part[xs, :, ys, :, mine]

    def all_sum(buf, n):
        total = buf[0]
        for i in range(1, n):
            total = total + buf[i]
        return total

    pos1 = x * (1 - c) + y * c
    pos2 = y * (1 - c) + x * c

    def on1(d):
        return {"x": lax.rem(x + d * (1 - c), NX), "y": lax.rem(y + d * c, NY)}

    def on2(d):
        return {"x": lax.rem(x + d * c, NX), "y": lax.rem(y + d * (1 - c), NY)}

    up1, dn1 = lax.rem(pos1 + 1, 4), lax.rem(pos1 + 3, 4)
    far1 = lax.rem(pos1 + 2, 4)
    up2, dn2 = lax.rem(pos2 + 1, 4), lax.rem(pos2 + 3, 4)
    far2 = lax.rem(pos2 + 2, 4)
    H0, H1 = pl.ds(0, 4), pl.ds(4, 4)

    for b in range(4):
        take(far1, b)
    m1p = copy(own.at[far1, :, H0], b1p, r1_send.at[0], r1_recv.at[0], **on1(1))
    m1m = copy(own.at[far1, :, H1], b1m, r1_send.at[1], r1_recv.at[1], **on1(3))
    m1p.start()
    m1m.start()
    for b in range(4):
        take(up1, b)
    mdp = copy(own.at[up1, :, H1], bdp, r1_send.at[2], r1_recv.at[2], **on1(1))
    mdp.start()
    for b in range(4):
        take(dn1, b)
    mdm = copy(own.at[dn1, :, H0], bdm, r1_send.at[3], r1_recv.at[3], **on1(3))
    mdm.start()
    for b in range(4):
        take(pos1, b)
    sc.wait_recv()
    s_x[x] = all_sum(s_c, 2)
    sx = []
    for d in range(1, NX):
        cp = copy(s_x.at[x], s_x.at[x], sx_send.at[d], sx_recv.at[d], x=lax.rem(x + d, NX))
        cp.start()
        sx.append(cp)

    fill(1)

    m1p.wait_recv()
    own[up1, :, H0] = own[up1, :, H0] + b1p[...]
    m2p = copy(own.at[up1, :, H0], b2p, r1_send.at[4], r1_recv.at[4], **on1(1))
    m2p.start()
    m1m.wait_recv()
    own[dn1, :, H1] = own[dn1, :, H1] + b1m[...]
    m2m = copy(own.at[dn1, :, H1], b2m, r1_send.at[5], r1_recv.at[5], **on1(3))
    m2m.start()

    for cp in sx:
        cp.wait_recv()
    s_y[y] = all_sum(s_x, NX)
    sy = []
    for d in range(1, NY):
        cp = copy(s_y.at[y], s_y.at[y], sy_send.at[d], sy_recv.at[d], y=lax.rem(y + d, NY))
        cp.start()
        sy.append(cp)

    fill(2)

    mdm.wait_recv()
    mdp.wait_recv()
    m2p.wait_recv()
    mid[:, H0] = own[pos1, :, H0] + b2p[...] + bdm[...]
    m2m.wait_recv()
    mid[:, H1] = own[pos1, :, H1] + b2m[...] + bdp[...]

    n1p = copy(mid.at[far2, H0], c1p, r2_send.at[0], r2_recv.at[0], **on2(1))
    n1m = copy(mid.at[far2, H1], c1m, r2_send.at[1], r2_recv.at[1], **on2(3))
    ndp = copy(mid.at[up2, H1], cdp, r2_send.at[2], r2_recv.at[2], **on2(1))
    ndm = copy(mid.at[dn2, H0], cdm, r2_send.at[3], r2_recv.at[3], **on2(3))
    for cp in (n1p, n1m, ndp, ndm):
        cp.start()

    for cp in sy:
        cp.wait_recv()
    s_z[z] = all_sum(s_y, NY)
    sz = []
    for d in range(1, NZ):
        cp = copy(s_z.at[z], s_z.at[z], sz_send.at[d], sz_recv.at[d], z=lax.rem(z + d, NZ))
        cp.start()
        sz.append(cp)

    fill(3)

    n1p.wait_recv()
    mid[up2, H0] = mid[up2, H0] + c1p[...]
    n2p = copy(mid.at[up2, H0], c2p, r2_send.at[4], r2_recv.at[4], **on2(1))
    n2p.start()
    n1m.wait_recv()
    mid[dn2, H1] = mid[dn2, H1] + c1m[...]
    n2m = copy(mid.at[dn2, H1], c2m, r2_send.at[5], r2_recv.at[5], **on2(3))
    n2m.start()

    fill(4)

    ndm.wait_recv()
    ndp.wait_recv()
    n2p.wait_recv()
    low[H0] = mid[pos2, H0] + c2p[...] + cdm[...]
    n2m.wait_recv()
    low[H1] = mid[pos2, H1] + c2m[...] + cdp[...]

    zs = []
    for d in range(1, NZ):
        to = lax.rem(z + d, NZ)
        cp = copy(low.at[to], zin.at[z], z_send.at[d], z_recv.at[d], z=to)
        cp.start()
        zs.append(cp)
    zin[z] = low[z]

    fill(5)

    for cp in sz:
        cp.wait_recv()
    total = all_sum(s_z, NZ)
    count = total[1:2]
    mean = total[0:1] / count
    mean_ref[...] = mean
    base = x * 256 + z * 32 + y * 8
    lane = lax.broadcasted_iota(jnp.int32, (8, DIM), 1)
    row = lax.broadcasted_iota(jnp.int32, (8, DIM), 0)
    mean_col = jnp.sum(jnp.where(lane == base + row, jnp.broadcast_to(mean, (8, DIM)), 0.0), axis=1, keepdims=True)
    outer = mean_col * mean
    cov_ref[0:8, :] = outer

    for cp in zs:
        cp.wait_recv()
    second = all_sum(zin, NZ)
    gath[y, c] = second / count[:, 0:1] - cov_ref[0:8, mine]
    gs = []
    k = 0
    for dy in range(NY):
        for dc in range(2):
            if dy + dc == 0:
                continue
            cp = copy(
                gath.at[y, c], gath.at[y, c], g_send.at[k], g_recv.at[k],
                y=lax.rem(y + dy, NY), c=(sib if dc else c),
            )
            cp.start()
            gs.append(cp)
            k += 1

    fill(6)
    rollout(done, STEPS // PACK - done) if done < STEPS // PACK else None
    scaled = acc[...] * (rv_ref[...] * (1.0 / STEPS))
    folded = scaled[:, :128] + scaled[:, 128:]
    ret_ref[...] = jnp.sum(folded.T, axis=0, keepdims=True)

    for cp in gs:
        cp.wait_recv()
    for ys in range(NY):
        for cc in range(2):
            cov_ref[ys * 8:(ys + 1) * 8, cc * HALF:(cc + 1) * HALF] = gath[ys, cc]

    for cp in pair + [sc, m1p, m1m, mdp, mdm, m2p, m2m, n1p, n1m, ndp, ndm, n2p, n2m] + sx + sy + sz + zs + gs:
        cp.wait_send()


def on_device(actions, elite_mask, init_state, w_state, w_action, bias, w_out, reward_vec):
    cand = actions.shape[0]
    f32 = jnp.float32
    vmem = pl.BlockSpec(memory_space=pltpu.VMEM)
    dma = pltpu.SemaphoreType.DMA
    V = pltpu.VMEM
    big = (4, 4, 8, HALF)
    small = (4, 8, HALF)
    scratch = (
        [V((NX, NZ, NY, 8, DIM), f32), V((4, 4, NZ, 8, HALF), f32)]
        + [V(big, f32)] * 6
        + [V((4, NZ, 8, HALF), f32)]
        + [V(small, f32)] * 6
        + [V((NZ, 8, HALF), f32), V((NZ, 8, HALF), f32), V((NY, 2, 8, HALF), f32)]
        + [V((n, 2, DIM), f32) for n in (2, NX, NY, NZ)]
        + [V((PACK, 128, STATE), jnp.bfloat16), V((cand, STATE), f32), V((cand, STATE), f32)]
        + [dma((16,)), dma((16,)), dma((6,)), dma((6,)), dma((6,)), dma((6,)), dma((NZ,)), dma((NZ,)), dma((7,)), dma((7,))]
        + [dma(()), dma(()), dma((NX,)), dma((NX,)), dma((NY,)), dma((NY,)), dma((NZ,)), dma((NZ,))]
    )
    mean, cov, ret = pl.pallas_call(
        kernel,
        out_shape=(
            jax.ShapeDtypeStruct((1, DIM), f32),
            jax.ShapeDtypeStruct((32, DIM), f32),
            jax.ShapeDtypeStruct((1, cand), f32),
        ),
        in_specs=[vmem] * 8,
        out_specs=[vmem] * 3,
        scratch_shapes=scratch,
        compiler_params=pltpu.CompilerParams(collective_id=0, has_side_effects=True, vmem_limit_bytes=48 * 1024 * 1024),
    )(
        actions, elite_mask.reshape(1, cand), init_state.reshape(1, STATE), w_state, w_action,
        bias.reshape(1, STATE), w_out, reward_vec.reshape(1, STATE),
    )
    return mean.reshape(DIM), cov, ret.reshape(cand)


def solution(mesh):
    torus = Mesh(mesh.devices.reshape(NX, NZ, NY, 2), AXES)
    placed = (P(AXES, None), P(AXES), P(), P(), P(), P(), P(), P())
    return jax.shard_map(
        on_device,
        mesh=torus,
        in_specs=placed,
        out_specs=(P(), P(("x", "z"), None), P(AXES)),
        check_vma=False,
    )
```

```python
import jax
import jax.numpy as jnp
from jax import lax
from jax.experimental import pallas as pl
from jax.experimental.pallas import tpu as pltpu
from jax.sharding import Mesh
from jax.sharding import PartitionSpec as P

ACT = 32
STEPS = 32
STATE = 256
DIM = 1024
MESH = pl.DeviceIdType.MESH
AXES = ("x", "z", "y", "c")
NX, NZ, NY = 4, 8, 4
PACK = 128 // ACT
FILL = (3, 10, 9, 4, 4, 2)


def kernel(
    act_hbm, mask_hbm, init_hbm, ws_hbm, wa_hbm, bias_hbm, wo_hbm, rv_hbm,
    mean_ref, cov_ref, ret_ref,
    act, mask, init, ws, wa, bias, wo, rv,
    at, part, own, b1p, b1m, bdp, bdm, b2p, b2m, mid, c1p, c1m, cdp, cdm, c2p, c2m, low, zin, gath,
    s_c, s_x, s_y, s_z, wa_pad, state, acc,
    load_sem, hello,
    pair_send, pair_recv, r1_send, r1_recv, r2_send, r2_recv, z_send, z_recv, g_send, g_recv,
    sc_send, sc_recv, sx_send, sx_recv, sy_send, sy_recv, sz_send, sz_recv,
):
    x, z, y, c = (lax.axis_index(a) for a in AXES)
    sib = 1 - c
    f32, bf16 = jnp.float32, jnp.bfloat16

    def at_x(d):
        return {"x": lax.rem(x + d, NX)}

    def at_y(d):
        return {"y": lax.rem(y + d, NY)}

    def at_z(d):
        return {"z": lax.rem(z + d, NZ)}

    def copy(src, dst, ssem, rsem, where):
        return pltpu.make_async_remote_copy(
            src_ref=src, dst_ref=dst, send_sem=ssem, recv_sem=rsem,
            device_id=where, device_id_type=MESH,
        )

    def signal(sem, where):
        pl.semaphore_signal(sem, inc=1, device_id=where, device_id_type=MESH)

    near = [{"c": sib}, at_x(1), at_x(3), at_y(1), at_y(3), at_z(1), at_z(NZ - 1)]
    barrier = pltpu.get_barrier_semaphore()
    for where in near:
        signal(barrier, where)

    rows = act_hbm.shape[0] // 4
    loads = [
        pltpu.make_async_copy(act_hbm.at[pl.ds(i * rows, rows)], act.at[pl.ds(i * rows, rows)], load_sem.at[i])
        for i in range(4)
    ]
    for i, (src, dst) in enumerate((
        (mask_hbm, mask), (init_hbm, init), (ws_hbm, ws), (wa_hbm, wa), (bias_hbm, bias), (wo_hbm, wo), (rv_hbm, rv)
    )):
        loads.append(pltpu.make_async_copy(src, dst, load_sem.at[4 + i]))
    for cp in loads:
        cp.start()
    for cp in loads[:5]:
        cp.wait()

    w_row = mask[...].astype(f32)
    w_b = w_row.astype(bf16)
    for xs in range(NX):
        at[xs * 256:(xs + 1) * 256, :] = act[:, xs * 256:(xs + 1) * 256].T * w_b

    pos1 = x * (1 - c) + y * c
    pos2 = y * (1 - c) + x * c
    sib1 = y * (1 - c) + x * c

    def on1(d):
        return {"x": lax.rem(x + d * (1 - c), NX), "y": lax.rem(y + d * c, NY)}

    def on2(d):
        return {"x": lax.rem(x + d * c, NX), "y": lax.rem(y + d * (1 - c), NY)}

    def ring(pos):
        return lax.rem(pos + 1, 4), lax.rem(pos + 2, 4), lax.rem(pos + 3, 4)

    up1, far1, dn1 = ring(pos1)
    up2, far2, dn2 = ring(pos2)
    far_sib = lax.rem(sib1 + 2, 4)

    def product(core, pair):
        for i in range(4):
            xs = (2 * pair + i // 2) * (1 - core) + i * core
            half = (i % 2) * (1 - core) + pair * core
            left = at[pl.ds(pl.multiple_of(xs * 256, 256), 256), :]
            right = act[:, pl.ds(pl.multiple_of(core * 512 + half * 256, 256), 256)]
            prod = jnp.dot(left, right, preferred_element_type=f32)
            for k in range(2):
                part[core, xs, 2 * half + k] = prod[:, k * 128:(k + 1) * 128]

    def pair_copy(core, a, b):
        xs = a * (1 - core) + b * core
        ys = b * (1 - core) + a * core
        return copy(part.at[core, xs, ys], own.at[a, b], pair_send.at[a * 4 + b], pair_recv.at[a * 4 + b], {"c": sib})

    def give(a):
        for b in range(4):
            cp = pair_copy(sib, a, b)
            cp.start()

    def other(a):
        return a + 1 - 2 * lax.rem(a, 2)

    pair_sib = lax.div(far_sib, 2)
    pair_own = lax.div(far1, 2)
    product(sib, pair_sib)
    pl.semaphore_wait(barrier, len(near))
    give(far_sib)
    give(other(far_sib))
    for where in near:
        signal(hello.at[0], where)

    sums = jnp.dot(jnp.broadcast_to(w_b, (16, w_b.shape[1])), act[...], preferred_element_type=f32)
    s_c[c, 0:1, :] = sums[0:1]
    s_c[c, 1:2, :] = jnp.broadcast_to(jnp.sum(w_row, axis=1, keepdims=True), (1, DIM))
    sc = copy(s_c.at[c], s_c.at[c], sc_send, sc_recv, {"c": sib})
    sc.start()

    product(c, pair_own)
    product(sib, 1 - pair_sib)
    give(lax.rem(far_sib + 2, 4))
    give(other(lax.rem(far_sib + 2, 4)))
    product(c, 1 - pair_own)

    for cp in loads[5:]:
        cp.wait()
    wa_pad[...] = jnp.zeros_like(wa_pad)
    for j in range(PACK):
        wa_pad[j, j * ACT:(j + 1) * ACT, :] = wa[...]
    state[...] = jnp.broadcast_to(init[...], state.shape)
    acc[...] = jnp.zeros_like(acc)
    done = 0

    def fill(k):
        nonlocal done
        count = min(FILL[k], STEPS - done) if k < len(FILL) else STEPS - done
        if count <= 0:
            return

        @pl.loop(done, done + count)
        def _(t):
            block = act[:, pl.ds(pl.multiple_of(lax.div(t, PACK) * 128, 128), 128)]
            st = state[...]
            pre = jnp.dot(st.astype(bf16), ws[...], preferred_element_type=f32)
            pre = pre + jnp.dot(block, wa_pad[lax.rem(t, PACK)], preferred_element_type=f32) + bias[...]
            hidden = jnp.tanh(pre).astype(bf16)
            st = 0.9 * st + jnp.dot(hidden, wo[...], preferred_element_type=f32)
            state[...] = st
            acc[...] += st

        done += count

    def take(a):
        for b in range(4):
            pair_copy(c, a, b).wait_recv()
            xs = a * (1 - c) + b * c
            ys = b * (1 - c) + a * c
            own[a, b] = own[a, b] + part[c, xs, ys]

    def all_sum(buf, n):
        total = buf[0]
        for i in range(1, n):
            total = total + buf[i]
        return total

    def spread(buf, pos, n, ssem, rsem, to):
        cps = []
        for d in range(1, n):
            cp = copy(buf.at[pos], buf.at[pos], ssem.at[d], rsem.at[d], to(d))
            cp.start()
            cps.append(cp)
        return cps

    H0, H1 = pl.ds(0, 128), pl.ds(128, 128)

    sc.wait_recv()
    s_x[x] = all_sum(s_c, 2)
    pl.semaphore_wait(hello.at[0], len(near))
    sx = spread(s_x, x, NX, sx_send, sx_recv, at_x)
    for where in near[3:]:
        signal(hello.at[1], where)

    take(far1)
    m1p = copy(own.at[far1, :, H0], b1p, r1_send.at[0], r1_recv.at[0], on1(1))
    m1m = copy(own.at[far1, :, H1], b1m, r1_send.at[1], r1_recv.at[1], on1(3))
    m1p.start()
    m1m.start()
    fill(0)
    take(other(far1))
    take(lax.rem(other(far1) + 2, 4))
    mdp = copy(own.at[up1, :, H1], bdp, r1_send.at[2], r1_recv.at[2], on1(1))
    mdm = copy(own.at[dn1, :, H0], bdm, r1_send.at[3], r1_recv.at[3], on1(3))
    mdp.start()
    mdm.start()
    take(pos1)

    fill(1)

    m1p.wait_recv()
    own[up1, :, H0] = own[up1, :, H0] + b1p[...]
    m2p = copy(own.at[up1, :, H0], b2p, r1_send.at[4], r1_recv.at[4], on1(1))
    m2p.start()
    m1m.wait_recv()
    own[dn1, :, H1] = own[dn1, :, H1] + b1m[...]
    m2m = copy(own.at[dn1, :, H1], b2m, r1_send.at[5], r1_recv.at[5], on1(3))
    m2m.start()

    pl.semaphore_wait(hello.at[1], 4)
    for where in near[3:]:
        signal(hello.at[2], where)
    fill(2)

    for cp in sx:
        cp.wait_recv()
    s_y[y] = all_sum(s_x, NX)

    mdm.wait_recv()
    mdp.wait_recv()
    m2p.wait_recv()
    mid[:, H0] = own[pos1, :, H0] + b2p[...] + bdm[...]
    n1p = copy(mid.at[far2, H0], c1p, r2_send.at[0], r2_recv.at[0], on2(1))
    n1p.start()
    m2m.wait_recv()
    mid[:, H1] = own[pos1, :, H1] + b2m[...] + bdp[...]
    n1m = copy(mid.at[far2, H1], c1m, r2_send.at[1], r2_recv.at[1], on2(3))
    n1m.start()
    sy = spread(s_y, y, NY, sy_send, sy_recv, at_y)
    ndp = copy(mid.at[up2, H1], cdp, r2_send.at[2], r2_recv.at[2], on2(1))
    ndm = copy(mid.at[dn2, H0], cdm, r2_send.at[3], r2_recv.at[3], on2(3))
    ndp.start()
    ndm.start()

    fill(3)

    n1p.wait_recv()
    mid[up2, H0] = mid[up2, H0] + c1p[...]
    n2p = copy(mid.at[up2, H0], c2p, r2_send.at[4], r2_recv.at[4], on2(1))
    n2p.start()
    n1m.wait_recv()
    mid[dn2, H1] = mid[dn2, H1] + c1m[...]
    n2m = copy(mid.at[dn2, H1], c2m, r2_send.at[5], r2_recv.at[5], on2(3))
    n2m.start()

    for cp in sy:
        cp.wait_recv()
    s_z[z] = all_sum(s_y, NY)
    pl.semaphore_wait(hello.at[2], 4)
    sz = spread(s_z, z, NZ, sz_send, sz_recv, at_z)

    fill(4)

    ndm.wait_recv()
    ndp.wait_recv()
    n2p.wait_recv()
    low[H0] = mid[pos2, H0] + c2p[...] + cdm[...]
    n2m.wait_recv()
    low[H1] = mid[pos2, H1] + c2m[...] + cdp[...]

    zs = []
    for d in (4, 3, 5, 2, 6, 1, 7):
        to = lax.rem(z + d, NZ)
        src = low.at[pl.ds(pl.multiple_of(to * 32, 32), 32)]
        cp = copy(src, zin.at[z], z_send.at[d], z_recv.at[d], {"z": to})
        cp.start()
        zs.append(cp)
    zin[z] = low[pl.ds(pl.multiple_of(z * 32, 32), 32), :]

    fill(5)

    for cp in sz:
        cp.wait_recv()
    total = all_sum(s_z, NZ)
    count = total[1:2]
    mean = total[0:1] / count
    mean_ref[...] = mean
    lane = lax.broadcasted_iota(jnp.int32, (32, DIM), 1)
    row = lax.broadcasted_iota(jnp.int32, (32, DIM), 0) + (x * 256 + z * 32)
    mean_col = jnp.sum(jnp.where(lane == row, jnp.broadcast_to(mean, (32, DIM)), 0.0), axis=1, keepdims=True)
    outer = mean_col * mean_ref[:, pl.ds(pl.multiple_of(c * 512 + y * 128, 128), 128)]

    for cp in zs:
        cp.wait_recv()
    gath[y, c] = all_sum(zin, NZ) / count[:, 0:1] - outer
    gs = []
    for k, (dy, dc) in enumerate(((2, 0), (2, 1), (1, 0), (1, 1), (3, 0), (3, 1), (0, 1))):
        where = {"y": lax.rem(y + dy, NY), "c": sib if dc else c}
        cp = copy(gath.at[y, c], gath.at[y, c], g_send.at[k], g_recv.at[k], where)
        cp.start()
        gs.append(cp)

    fill(6)
    scaled = acc[...] * (rv[...] * (1.0 / STEPS))
    folded = scaled[:, :128] + scaled[:, 128:]
    ret_ref[...] = jnp.sum(folded.T, axis=0, keepdims=True)

    for a in range(4):
        for b in range(4):
            pair_copy(sib, a, b).wait_send()
    for cp in [sc, m1p, m1m, mdp, mdm, m2p, m2m, n1p, n1m, ndp, ndm, n2p, n2m] + sx + sy + sz + zs:
        cp.wait_send()
    for cp in gs:
        cp.wait_recv()
    for ys in range(NY):
        for cc in range(2):
            cov_ref[:, cc * 512 + ys * 128:cc * 512 + (ys + 1) * 128] = gath[ys, cc]
    for cp in gs:
        cp.wait_send()


def write_out(mean, cov, ret, mean_hbm, cov_hbm, ret_hbm, sem):
    cps = [
        pltpu.make_async_copy(src, dst, sem.at[i])
        for i, (src, dst) in enumerate(((cov, cov_hbm), (mean, mean_hbm), (ret, ret_hbm)))
    ]
    for cp in cps:
        cp.start()
    for cp in cps:
        cp.wait()


def on_device(actions, elite_mask, init_state, w_state, w_action, bias, w_out, reward_vec):
    cand = actions.shape[0]
    f32, i32, bf16 = jnp.float32, jnp.int32, jnp.bfloat16
    vmem = pl.BlockSpec(memory_space=pltpu.VMEM)
    hbm = pl.BlockSpec(memory_space=pltpu.HBM)
    dma = pltpu.SemaphoreType.DMA
    V = pltpu.VMEM
    scratch = (
        [V((cand, DIM), bf16), V((1, cand), i32), V((1, STATE), f32), V((STATE, STATE), bf16), V((ACT, STATE), bf16)]
        + [V((1, STATE), f32), V((STATE, STATE), bf16), V((1, STATE), f32)]
        + [V((DIM, cand), bf16), V((2, 4, 4, 256, 128), f32), V((4, 4, 256, 128), f32)]
        + [V((4, 128, 128), f32)] * 6
        + [V((4, 256, 128), f32)]
        + [V((128, 128), f32)] * 6
        + [V((256, 128), f32), V((NZ, 32, 128), f32), V((NY, 2, 32, 128), f32)]
        + [V((n, 2, DIM), f32) for n in (2, NX, NY, NZ)]
        + [V((PACK, 128, STATE), bf16), V((cand, STATE), f32), V((cand, STATE), f32)]
        + [dma((11,)), pltpu.SemaphoreType.REGULAR((3,))]
        + [dma((16,)), dma((16,)), dma((6,)), dma((6,)), dma((6,)), dma((6,)), dma((NZ,)), dma((NZ,)), dma((7,)), dma((7,))]
        + [dma(()), dma(()), dma((NX,)), dma((NX,)), dma((NY,)), dma((NY,)), dma((NZ,)), dma((NZ,))]
    )
    shapes = (
        jax.ShapeDtypeStruct((1, DIM), f32),
        jax.ShapeDtypeStruct((32, DIM), f32),
        jax.ShapeDtypeStruct((1, cand), f32),
    )
    args = (
        actions, elite_mask.reshape(1, cand), init_state.reshape(1, STATE), w_state, w_action,
        bias.reshape(1, STATE), w_out, reward_vec.reshape(1, STATE),
    )
    found = pl.pallas_call(
        kernel,
        out_shape=shapes,
        in_specs=[hbm] * 8,
        out_specs=[vmem] * 3,
        scratch_shapes=scratch,
        compiler_params=pltpu.CompilerParams(collective_id=0, has_side_effects=True, vmem_limit_bytes=48 * 1024 * 1024),
    )(*(pltpu.with_memory_space_constraint(a, pltpu.HBM) for a in args))
    mean, cov, ret = pl.pallas_call(
        write_out, out_shape=shapes, in_specs=[vmem] * 3, out_specs=[hbm] * 3, scratch_shapes=[dma((3,))],
        compiler_params=pltpu.CompilerParams(vmem_limit_bytes=1024 * 1024),
    )(*found)
    return mean.reshape(DIM), cov, ret.reshape(cand)


def solution(mesh):
    torus = Mesh(mesh.devices.reshape(NX, NZ, NY, 2), AXES)
    placed = (P(AXES, None), P(AXES), P(), P(), P(), P(), P(), P())
    return jax.shard_map(
        on_device,
        mesh=torus,
        in_specs=placed,
        out_specs=(P(), P(("x", "z"), None), P(AXES)),
        check_vma=False,
    )
```

```python
import jax
import jax.numpy as jnp
from jax import lax
from jax.experimental import pallas as pl
from jax.experimental.pallas import tpu as pltpu
from jax.sharding import Mesh
from jax.sharding import PartitionSpec as P

ACT = 32
STEPS = 32
STATE = 256
DIM = 1024
MESH = pl.DeviceIdType.MESH
AXES = ("x", "z", "y", "c")
NX, NZ, NY = 4, 8, 4
PACK = 128 // ACT
FILL = (3, 2, 1, 1, 1, 2, 2, 2, 1, 5, 6, 6)


def kernel(
    act_hbm, mask_hbm, init_hbm, ws_hbm, wa_hbm, bias_hbm, wo_hbm, rv_hbm,
    mean_ref, cov_ref, ret_ref,
    act, mask, init, ws, wa, bias, wo, rv,
    at, part, own, b1p, b1m, bdp, bdm, b2p, b2m, mid, c1p, c1m, cdp, cdm, c2p, c2m, low, zin, gath,
    s_c, s_x, s_y, s_z, wa_pad, state, acc,
    load_sem, hello,
    pair_send, pair_recv, r1_send, r1_recv, r2_send, r2_recv, z_send, z_recv, g_send, g_recv,
    sc_send, sc_recv, sx_send, sx_recv, sy_send, sy_recv, sz_send, sz_recv,
):
    x, z, y, c = (lax.axis_index(a) for a in AXES)
    sib = 1 - c
    f32, bf16 = jnp.float32, jnp.bfloat16

    def at_x(d):
        return {"x": lax.rem(x + d, NX)}

    def at_y(d):
        return {"y": lax.rem(y + d, NY)}

    def at_z(d):
        return {"z": lax.rem(z + d, NZ)}

    def copy(src, dst, ssem, rsem, where):
        return pltpu.make_async_remote_copy(
            src_ref=src, dst_ref=dst, send_sem=ssem, recv_sem=rsem,
            device_id=where, device_id_type=MESH,
        )

    def signal(sem, where):
        pl.semaphore_signal(sem, inc=1, device_id=where, device_id_type=MESH)

    near = [{"c": sib}, at_x(1), at_x(3), at_y(1), at_y(3), at_z(1), at_z(NZ - 1)]
    barrier = pltpu.get_barrier_semaphore()
    for where in near:
        signal(barrier, where)

    rows = act_hbm.shape[0] // 4
    loads = [
        pltpu.make_async_copy(act_hbm.at[pl.ds(i * rows, rows)], act.at[pl.ds(i * rows, rows)], load_sem.at[i])
        for i in range(4)
    ]
    for i, (src, dst) in enumerate((
        (mask_hbm, mask), (init_hbm, init), (ws_hbm, ws), (wa_hbm, wa), (bias_hbm, bias), (wo_hbm, wo), (rv_hbm, rv)
    )):
        loads.append(pltpu.make_async_copy(src, dst, load_sem.at[4 + i]))
    for cp in loads:
        cp.start()
    for cp in loads[:5]:
        cp.wait()

    w_row = mask[...].astype(f32)
    w_b = w_row.astype(bf16)
    for xs in range(NX):
        at[xs * 256:(xs + 1) * 256, :] = act[:, xs * 256:(xs + 1) * 256].T * w_b

    pos1 = x * (1 - c) + y * c
    pos2 = y * (1 - c) + x * c
    sib1 = y * (1 - c) + x * c

    def on1(d):
        return {"x": lax.rem(x + d * (1 - c), NX), "y": lax.rem(y + d * c, NY)}

    def on2(d):
        return {"x": lax.rem(x + d * c, NX), "y": lax.rem(y + d * (1 - c), NY)}

    def ring(pos):
        return lax.rem(pos + 1, 4), lax.rem(pos + 2, 4), lax.rem(pos + 3, 4)

    up1, far1, dn1 = ring(pos1)
    up2, far2, dn2 = ring(pos2)
    far_sib = lax.rem(sib1 + 2, 4)

    def product(core, pair):
        for i in range(4):
            xs = (2 * pair + i // 2) * (1 - core) + i * core
            half = (i % 2) * (1 - core) + pair * core
            left = at[pl.ds(pl.multiple_of(xs * 256, 256), 256), :]
            right = act[:, pl.ds(pl.multiple_of(core * 512 + half * 256, 256), 256)]
            prod = jnp.dot(left, right, preferred_element_type=f32)
            for k in range(2):
                part[core, xs, 2 * half + k] = prod[:, k * 128:(k + 1) * 128]

    def pair_copy(core, a, b):
        xs = a * (1 - core) + b * core
        ys = b * (1 - core) + a * core
        return copy(part.at[core, xs, ys], own.at[a, b], pair_send.at[a * 4 + b], pair_recv.at[a * 4 + b], {"c": sib})

    def other(a):
        return a + 1 - 2 * lax.rem(a, 2)

    order = (far2, up2, dn2, pos2)
    order_sib = (far1, up1, dn1, pos1)

    def give(a):
        for b in order_sib:
            pair_copy(sib, a, b).start()

    sums = jnp.dot(jnp.broadcast_to(w_b, (16, w_b.shape[1])), act[...], preferred_element_type=f32)
    s_c[c, 0:1, :] = sums[0:1]
    s_c[c, 1:2, :] = jnp.broadcast_to(jnp.sum(w_row, axis=1, keepdims=True), (1, DIM))
    pair_sib = lax.div(far_sib, 2)
    pair_own = lax.div(far1, 2)
    product(sib, pair_sib)
    pl.semaphore_wait(barrier, len(near))
    sc = copy(s_c.at[c], s_c.at[c], sc_send, sc_recv, {"c": sib})
    sc.start()
    give(far_sib)
    give(other(far_sib))
    for where in near:
        signal(hello.at[0], where)

    product(c, pair_own)
    product(sib, 1 - pair_sib)
    give(lax.rem(far_sib + 2, 4))
    give(other(lax.rem(far_sib + 2, 4)))
    product(c, 1 - pair_own)

    for cp in loads[5:]:
        cp.wait()
    wa_pad[...] = jnp.zeros_like(wa_pad)
    for j in range(PACK):
        wa_pad[j, j * ACT:(j + 1) * ACT, :] = wa[...]
    state[...] = jnp.broadcast_to(init[...], state.shape)
    acc[...] = jnp.zeros_like(acc)
    done = 0

    def step(t):
        block = act[:, pl.ds(pl.multiple_of(lax.div(t, PACK) * 128, 128), 128)]
        st = state[...]
        pre = jnp.dot(st.astype(bf16), ws[...], preferred_element_type=f32)
        pre = pre + jnp.dot(block, wa_pad[lax.rem(t, PACK)], preferred_element_type=f32) + bias[...]
        hidden = jnp.tanh(pre).astype(bf16)
        st = 0.9 * st + jnp.dot(hidden, wo[...], preferred_element_type=f32)
        state[...] = st
        acc[...] += st

    def fill(k):
        nonlocal done
        count = min(FILL[k], STEPS - done)
        if count > 0:
            pl.loop(done, done + count)(step)
        done += count

    def take(a, b):
        pair_copy(c, a, b).wait_recv()
        xs = a * (1 - c) + b * c
        ys = b * (1 - c) + a * c
        own[a, b] = own[a, b] + part[c, xs, ys]

    def all_sum(buf, n):
        total = buf[0]
        for i in range(1, n):
            total = total + buf[i]
        return total

    def spread(buf, pos, n, ssem, rsem, to):
        cps = []
        for d in range(1, n):
            cp = copy(buf.at[pos], buf.at[pos], ssem.at[d], rsem.at[d], to(d))
            cp.start()
            cps.append(cp)
        return cps

    H0, H1 = pl.ds(0, 128), pl.ds(128, 128)

    sc.wait_recv()
    s_x[x] = all_sum(s_c, 2)
    pl.semaphore_wait(hello.at[0], len(near))
    sx = spread(s_x, x, NX, sx_send, sx_recv, at_x)
    for where in near[3:]:
        signal(hello.at[1], where)

    def ring1(src, a, rows, dst, kind, d):
        return [
            copy(src.at[a, b, rows], dst.at[b], r1_send.at[kind, k], r1_recv.at[kind, k], on1(d))
            for k, b in enumerate(order)
        ]

    m1p, m1m = ring1(own, far1, H0, b1p, 0, 1), ring1(own, far1, H1, b1m, 1, 3)
    mdp, mdm = ring1(own, up1, H1, bdp, 2, 1), ring1(own, dn1, H0, bdm, 3, 3)
    m2p, m2m = ring1(own, up1, H0, b2p, 4, 1), ring1(own, dn1, H1, b2m, 5, 3)

    for k, b in enumerate(order):
        take(far1, b)
        m1p[k].start()
        m1m[k].start()
    fill(0)
    for b in order:
        take(up1, b)
        take(dn1, b)
    mdp[0].start()
    mdm[0].start()
    for b in order:
        take(pos1, b)
    fill(1)

    for k, b in enumerate(order):
        m1p[k].wait_recv()
        own[up1, b, H0] = own[up1, b, H0] + b1p[b]
        m2p[k].start()
        m1m[k].wait_recv()
        own[dn1, b, H1] = own[dn1, b, H1] + b1m[b]
        m2m[k].start()
        if k < 3:
            mdp[k + 1].start()
            mdm[k + 1].start()
            fill(2 + k)

    pl.semaphore_wait(hello.at[1], 4)
    for where in near[3:]:
        signal(hello.at[2], where)
    for cp in sx:
        cp.wait_recv()
    s_y[y] = all_sum(s_x, NX)
    sy = spread(s_y, y, NY, sy_send, sy_recv, at_y)
    fill(5)

    def low_half(k, b):
        mdm[k].wait_recv()
        m2p[k].wait_recv()
        mid[b, H0] = own[pos1, b, H0] + b2p[b] + bdm[b]

    def high_half(k, b):
        mdp[k].wait_recv()
        m2m[k].wait_recv()
        mid[b, H1] = own[pos1, b, H1] + b2m[b] + bdp[b]

    low_half(0, far2)
    n1p = copy(mid.at[far2, H0], c1p, r2_send.at[0], r2_recv.at[0], on2(1))
    n1p.start()
    high_half(0, far2)
    n1m = copy(mid.at[far2, H1], c1m, r2_send.at[1], r2_recv.at[1], on2(3))
    n1m.start()
    fill(6)
    high_half(1, up2)
    ndp = copy(mid.at[up2, H1], cdp, r2_send.at[2], r2_recv.at[2], on2(1))
    ndp.start()
    low_half(1, up2)
    fill(7)
    low_half(2, dn2)
    ndm = copy(mid.at[dn2, H0], cdm, r2_send.at[3], r2_recv.at[3], on2(3))
    ndm.start()
    high_half(2, dn2)
    fill(8)

    n1p.wait_recv()
    mid[up2, H0] = mid[up2, H0] + c1p[...]
    n2p = copy(mid.at[up2, H0], c2p, r2_send.at[4], r2_recv.at[4], on2(1))
    n2p.start()
    n1m.wait_recv()
    mid[dn2, H1] = mid[dn2, H1] + c1m[...]
    n2m = copy(mid.at[dn2, H1], c2m, r2_send.at[5], r2_recv.at[5], on2(3))
    n2m.start()

    for cp in sy:
        cp.wait_recv()
    s_z[z] = all_sum(s_y, NY)
    pl.semaphore_wait(hello.at[2], 4)
    sz = spread(s_z, z, NZ, sz_send, sz_recv, at_z)
    low_half(3, pos2)
    high_half(3, pos2)

    fill(9)

    ndm.wait_recv()
    ndp.wait_recv()
    n2p.wait_recv()
    low[H0] = mid[pos2, H0] + c2p[...] + cdm[...]
    n2m.wait_recv()
    low[H1] = mid[pos2, H1] + c2m[...] + cdp[...]

    zs = []
    for d in (4, 3, 5, 2, 6, 1, 7):
        to = lax.rem(z + d, NZ)
        src = low.at[pl.ds(pl.multiple_of(to * 32, 32), 32)]
        cp = copy(src, zin.at[z], z_send.at[d], z_recv.at[d], {"z": to})
        cp.start()
        zs.append(cp)
    zin[z] = low[pl.ds(pl.multiple_of(z * 32, 32), 32), :]

    fill(10)

    for cp in sz:
        cp.wait_recv()
    total = all_sum(s_z, NZ)
    count = total[1:2]
    mean = total[0:1] / count
    mean_ref[...] = mean
    lane = lax.broadcasted_iota(jnp.int32, (32, DIM), 1)
    row = lax.broadcasted_iota(jnp.int32, (32, DIM), 0) + (x * 256 + z * 32)
    mean_col = jnp.sum(jnp.where(lane == row, jnp.broadcast_to(mean, (32, DIM)), 0.0), axis=1, keepdims=True)
    outer = mean_col * mean_ref[:, pl.ds(pl.multiple_of(c * 512 + y * 128, 128), 128)]

    for cp in zs:
        cp.wait_recv()
    gath[y, c] = all_sum(zin, NZ) / count[:, 0:1] - outer
    gs = []
    for k, (dy, dc) in enumerate(((2, 0), (2, 1), (1, 0), (1, 1), (3, 0), (3, 1), (0, 1))):
        where = {"y": lax.rem(y + dy, NY), "c": sib if dc else c}
        cp = copy(gath.at[y, c], gath.at[y, c], g_send.at[k], g_recv.at[k], where)
        cp.start()
        gs.append(cp)

    fill(11)
    assert done == STEPS
    scaled = acc[...] * (rv[...] * (1.0 / STEPS))
    folded = scaled[:, :128] + scaled[:, 128:]
    ret_ref[...] = jnp.sum(folded.T, axis=0, keepdims=True)

    for a in range(4):
        for b in range(4):
            pair_copy(sib, a, b).wait_send()
    for cp in m1p + m1m + mdp + mdm + m2p + m2m + [sc, n1p, n1m, ndp, ndm, n2p, n2m] + sx + sy + sz + zs:
        cp.wait_send()
    for cp in gs:
        cp.wait_recv()
    for ys in range(NY):
        for cc in range(2):
            cov_ref[:, cc * 512 + ys * 128:cc * 512 + (ys + 1) * 128] = gath[ys, cc]
    for cp in gs:
        cp.wait_send()


def write_out(mean, cov, ret, mean_hbm, cov_hbm, ret_hbm, sem):
    cps = [
        pltpu.make_async_copy(src, dst, sem.at[i])
        for i, (src, dst) in enumerate(((cov, cov_hbm), (mean, mean_hbm), (ret, ret_hbm)))
    ]
    for cp in cps:
        cp.start()
    for cp in cps:
        cp.wait()


def on_device(actions, elite_mask, init_state, w_state, w_action, bias, w_out, reward_vec):
    cand = actions.shape[0]
    f32, i32, bf16 = jnp.float32, jnp.int32, jnp.bfloat16
    vmem = pl.BlockSpec(memory_space=pltpu.VMEM)
    hbm = pl.BlockSpec(memory_space=pltpu.HBM)
    dma = pltpu.SemaphoreType.DMA
    V = pltpu.VMEM
    scratch = (
        [V((cand, DIM), bf16), V((1, cand), i32), V((1, STATE), f32), V((STATE, STATE), bf16), V((ACT, STATE), bf16)]
        + [V((1, STATE), f32), V((STATE, STATE), bf16), V((1, STATE), f32)]
        + [V((DIM, cand), bf16), V((2, 4, 4, 256, 128), f32), V((4, 4, 256, 128), f32)]
        + [V((4, 128, 128), f32)] * 6
        + [V((4, 256, 128), f32)]
        + [V((128, 128), f32)] * 6
        + [V((256, 128), f32), V((NZ, 32, 128), f32), V((NY, 2, 32, 128), f32)]
        + [V((n, 2, DIM), f32) for n in (2, NX, NY, NZ)]
        + [V((PACK, 128, STATE), bf16), V((cand, STATE), f32), V((cand, STATE), f32)]
        + [dma((11,)), pltpu.SemaphoreType.REGULAR((3,))]
        + [dma((16,)), dma((16,)), dma((6, 4)), dma((6, 4)), dma((6,)), dma((6,)), dma((NZ,)), dma((NZ,)), dma((7,)), dma((7,))]
        + [dma(()), dma(()), dma((NX,)), dma((NX,)), dma((NY,)), dma((NY,)), dma((NZ,)), dma((NZ,))]
    )
    shapes = (
        jax.ShapeDtypeStruct((1, DIM), f32),
        jax.ShapeDtypeStruct((32, DIM), f32),
        jax.ShapeDtypeStruct((1, cand), f32),
    )
    args = (
        actions, elite_mask.reshape(1, cand), init_state.reshape(1, STATE), w_state, w_action,
        bias.reshape(1, STATE), w_out, reward_vec.reshape(1, STATE),
    )
    found = pl.pallas_call(
        kernel,
        out_shape=shapes,
        in_specs=[hbm] * 8,
        out_specs=[vmem] * 3,
        scratch_shapes=scratch,
        compiler_params=pltpu.CompilerParams(collective_id=0, has_side_effects=True, vmem_limit_bytes=48 * 1024 * 1024),
    )(*(pltpu.with_memory_space_constraint(a, pltpu.HBM) for a in args))
    mean, cov, ret = pl.pallas_call(
        write_out, out_shape=shapes, in_specs=[vmem] * 3, out_specs=[hbm] * 3, scratch_shapes=[dma((3,))],
        compiler_params=pltpu.CompilerParams(vmem_limit_bytes=1024 * 1024),
    )(*found)
    return mean.reshape(DIM), cov, ret.reshape(cand)


def solution(mesh):
    torus = Mesh(mesh.devices.reshape(NX, NZ, NY, 2), AXES)
    placed = (P(AXES, None), P(AXES), P(), P(), P(), P(), P(), P())
    return jax.shard_map(
        on_device,
        mesh=torus,
        in_specs=placed,
        out_specs=(P(), P(("x", "z"), None), P(AXES)),
        check_vma=False,
    )
```
